32 devices in a mesh: layer: 4 (over z), facet: 8 (over y, x, core).
Axes of the slice: x: 2, y: 2, z: 4, core: 2. Of those that a mesh axis runs over, the one named last changes fastest.
Arguments:
- model_strip: bfloat16 [8, 2, 64, 8192], P('facet', None, None, 'layer'), may hold values from -6 to 6
- screen_angle: bfloat16 [4, 8, 64, 8192], P('layer', 'facet'), may hold values from -3.140625 to 3.140625
- facet_window: float32 [8, 8192], P('facet'), may hold values from 0.04 to 0.16
- facet_shift: int32 [8], P('facet'), may hold values from 0 to 8191
- kernel_taps: float32 [7], replicated, may hold values from 0.2 to 0.6
- plane_angle: float32 [4, 8], P('layer'), may hold values from -3.140625 to 3.140625
- u_cell: int32 [4, 128, 512], P('layer', 'facet'), may hold values from 0 to 63
- v_cell: int32 [4, 128, 512], P('layer', 'facet'), may hold values from 0 to 63
- w_plane: int32 [4, 128, 512], P('layer', 'facet'), may hold values from 0 to 7
- observed: float32 [4, 128, 2, 512], P('layer', 'facet'), may hold values from -6 to 6
Outputs:
- residual: float32 [4, 128, 2, 512], P('layer', 'facet')
- gradient: float32 [8, 2, 64, 8192], P('facet', None, None, 'layer')
The draws below stay inside these ranges and needn't reach their ends.
All inputs are finite; a program needn't handle non-finite values.
Results may differ from the reference program's by a relative error of at most 0.009.
Values may be sent and summed in bfloat16 or wider, within the bound.
A program may use at most 64 MiB of HBM per device.

```python
import math
import jax
import jax.numpy as jnp
from jax import lax

STRIP_LEN = 8192
SUB_ROWS = 64
STRIP_COLS = 64
VIS = 512
PLANES = 8
TAPS = 7
SUBGRIDS = 128
LAYERS = 4
FACETS = 8


def touch_ends(entries, rng, low, largest):
    extent = entries.shape
    place = [jax.random.randint(jax.random.fold_in(rng, axis), (), 0, extent[axis]) for axis in range(len(extent))]
    entries = entries.at[tuple(place)].set(low)
    longest = extent.index(max(extent))
    place[longest] = (place[longest] + 1) % extent[longest]
    return entries.at[tuple(place)].set(largest)


def steps_of(stream_key, extent, shards, low, high):
    gain, own = 1.0, jax.random.fold_in(stream_key, 6)
    for dim, shards_of in shards:
        draws = jnp.exp(jax.random.uniform(jax.random.fold_in(own, dim), (shards_of,), jnp.float32, low / len(shards), high / len(shards)))
        gain = gain * jnp.repeat(draws, extent[dim] // shards_of).reshape([-1 if axis == dim else 1 for axis in range(len(extent))])
    return gain


def noise(stream_key, extent, deviation, reach, cuts=(), kind=jnp.bfloat16):
    factor_of = steps_of(stream_key, extent, cuts, -0.22, 0.18) if cuts else 1.0
    array = jax.random.normal(stream_key, extent, jnp.float32) * deviation * factor_of
    return jnp.minimum(jnp.maximum(array, -reach), reach).astype(kind)


def setup_inputs(seed: int = 0) -> dict:
    arg_keys = jax.random.split(jax.random.key(seed), 11)
    return {
        "model_strip": noise(arg_keys[0], (FACETS, 2, STRIP_COLS, STRIP_LEN), 1.0, 6.0, ((0, 8), (3, 4))),
        "screen_angle": jnp.clip(jax.random.uniform(arg_keys[1], (LAYERS, FACETS, STRIP_COLS, STRIP_LEN), jnp.float32, -3.140625, 3.140625), -3.140625, 3.140625).astype(jnp.bfloat16),
        "facet_window": jnp.clip(jnp.exp(math.log(0.16) - 1.3862944 * jax.random.uniform(arg_keys[2], (FACETS, STRIP_LEN), jnp.float32) ** steps_of(arg_keys[2], (FACETS, STRIP_LEN), ((0, 8),), -0.2, 0.2)), 0.04, 0.16),
        "facet_shift": touch_ends(jax.random.randint(arg_keys[3], (FACETS,), 0, STRIP_LEN), jax.random.fold_in(arg_keys[3], 1), 0, STRIP_LEN - 1).astype(jnp.int32),
        "kernel_taps": jnp.clip(jax.random.uniform(arg_keys[4], (TAPS,), jnp.float32, 0.2, 0.6), 0.2, 0.6),
        "plane_angle": jnp.clip(jax.random.uniform(arg_keys[5], (LAYERS, PLANES), jnp.float32, -3.140625, 3.140625), -3.140625, 3.140625),
        "u_cell": touch_ends(jax.random.randint(arg_keys[6], (LAYERS, SUBGRIDS, VIS), 0, SUB_ROWS), jax.random.fold_in(arg_keys[6], 1), 0, SUB_ROWS - 1).astype(jnp.int32),
        "v_cell": touch_ends(jax.random.randint(arg_keys[7], (LAYERS, SUBGRIDS, VIS), 0, STRIP_COLS), jax.random.fold_in(arg_keys[7], 1), 0, STRIP_COLS - 1).astype(jnp.int32),
        "w_plane": touch_ends(jax.random.randint(arg_keys[8], (LAYERS, SUBGRIDS, VIS), 0, PLANES), jax.random.fold_in(arg_keys[8], 1), 0, PLANES - 1).astype(jnp.int32),
        "observed": noise(arg_keys[9], (LAYERS, SUBGRIDS, 2, VIS), 1.0, 6.0, ((0, 4), (1, 8)), jnp.float32),
    }


back_gain = 8.0

def fourier_table(length):
    positions = jnp.arange(length, dtype=jnp.int32)
    turn_count = positions[:, None] * positions[None, :] % length
    angles = 2.0 * math.pi / length * turn_count.astype(jnp.float32)
    norm_scale = 1.0 / math.sqrt(length)
    return (jnp.stack([jnp.cos(angles), -jnp.sin(angles)]) * norm_scale).astype(jnp.bfloat16)

def twiddle():
    low_index = jnp.arange(SUB_ROWS, dtype=jnp.int32)
    high_index = jnp.arange(SUBGRIDS, dtype=jnp.int32)
    turn_count = low_index[:, None] * high_index[None, :] % STRIP_LEN
    angles = 2.0 * math.pi / STRIP_LEN * turn_count.astype(jnp.float32)
    return (jnp.cos(angles), -jnp.sin(angles))

def facet_factor(window, shift_cells):
    positions = jnp.arange(STRIP_LEN, dtype=jnp.int32)
    turn_count = positions * shift_cells.astype(jnp.int32) % STRIP_LEN
    angles = 2.0 * math.pi / STRIP_LEN * turn_count.astype(jnp.float32)
    factor_real = (window * jnp.cos(angles)).reshape(SUBGRIDS, SUB_ROWS, 1)
    factor_imag = (-window * jnp.sin(angles)).reshape(SUBGRIDS, SUB_ROWS, 1)
    return (factor_real, factor_imag)

def forward(screened, window, shift_cells):
    grid_view = screened.reshape(2, STRIP_COLS, SUB_ROWS, SUBGRIDS).astype(jnp.float32)
    section_one = jnp.einsum('tka,pcab->tpckb', fourier_table(SUB_ROWS).astype(jnp.float32), grid_view)
    real_part = section_one[0, 0] - section_one[1, 1]
    imag_part = section_one[0, 1] + section_one[1, 0]
    twist_real, twist_imag = twiddle()
    mixed = jnp.stack([real_part * twist_real - imag_part * twist_imag, real_part * twist_imag + imag_part * twist_real]).astype(jnp.bfloat16)
    section_two = jnp.einsum('tjb,pckb->tpjkc', fourier_table(SUBGRIDS).astype(jnp.float32), mixed.astype(jnp.float32))
    spec_real = section_two[0, 0] - section_two[1, 1]
    spec_imag = section_two[0, 1] + section_two[1, 0]
    factor_real, factor_imag = facet_factor(window, shift_cells)
    return jnp.concatenate([spec_real * factor_real - spec_imag * factor_imag, spec_real * factor_imag + spec_imag * factor_real], axis=2).astype(jnp.bfloat16)

def backward(all_grids, window, shift_cells, screen_phase):
    values = all_grids.astype(jnp.float32)
    grid_real = values[:, :, :STRIP_COLS]
    grid_imag = values[:, :, STRIP_COLS:]
    factor_real, factor_imag = facet_factor(window, shift_cells)
    spectral = jnp.stack([grid_real * factor_real + grid_imag * factor_imag, grid_imag * factor_real - grid_real * factor_imag]).astype(jnp.bfloat16)
    section_two = jnp.einsum('tjb,pjkc->tpckb', fourier_table(SUBGRIDS).astype(jnp.float32), spectral.astype(jnp.float32))
    half_real = section_two[0, 0] + section_two[1, 1]
    half_imag = section_two[0, 1] - section_two[1, 0]
    twist_real, twist_imag = twiddle()
    mixed = jnp.stack([half_real * twist_real + half_imag * twist_imag, half_imag * twist_real - half_real * twist_imag]).astype(jnp.bfloat16)
    section_one = jnp.einsum('tka,pckb->tpcab', fourier_table(SUB_ROWS).astype(jnp.float32), mixed.astype(jnp.float32))
    image_real = (section_one[0, 0] + section_one[1, 1]).reshape(STRIP_COLS, STRIP_LEN)
    image_imag = (section_one[0, 1] - section_one[1, 0]).reshape(STRIP_COLS, STRIP_LEN)
    phases = screen_phase.astype(jnp.float32)
    cosine = jnp.cos(phases)
    sine_part = jnp.sin(phases)
    return back_gain * jnp.stack([image_real * cosine + image_imag * sine_part, image_imag * cosine - image_real * sine_part])

def spread(cell_index, length, kernel_taps):
    tap_count = kernel_taps.shape[0]
    offset = (jnp.arange(length, dtype=jnp.int32)[None, :] - cell_index[:, None]) % length
    wanted = (jnp.arange(tap_count, dtype=jnp.int32) - tap_count // 2) % length
    matches = (offset[:, :, None] == wanted[None, None, :]).astype(jnp.float32)
    return lax.optimization_barrier(jnp.sum(matches * kernel_taps, axis=2))

def degrid(subgrid, row_cells, column_cells, plane, observed_vis, angle_table, kernel_taps):
    row_weights = spread(row_cells, SUB_ROWS, kernel_taps)
    column_weights = spread(column_cells, STRIP_COLS, kernel_taps)
    kernel_rows = jnp.dot(row_weights, subgrid, precision=lax.Precision.HIGHEST)
    model_real = lax.optimization_barrier(jnp.sum(kernel_rows[:, :STRIP_COLS] * column_weights, axis=1))
    model_imag = lax.optimization_barrier(jnp.sum(kernel_rows[:, STRIP_COLS:] * column_weights, axis=1))
    plane_pick = (plane[:, None] == jnp.arange(PLANES, dtype=jnp.int32)[None, :]).astype(jnp.float32)
    phase_angle = lax.optimization_barrier(jnp.sum(plane_pick * angle_table[None, :], axis=1))
    cosine = jnp.cos(phase_angle)
    sine_part = jnp.sin(phase_angle)
    residual_real = observed_vis[0] - (model_real * cosine - model_imag * sine_part)
    residual_imag = observed_vis[1] - (model_real * sine_part + model_imag * cosine)
    weighted = jnp.stack([residual_real * cosine + residual_imag * sine_part, residual_imag * cosine - residual_real * sine_part])
    spread_cols = jnp.concatenate([weighted[0][:, None] * column_weights, weighted[1][:, None] * column_weights], axis=1)
    adjoint = jnp.dot(row_weights.T, spread_cols, precision=lax.Precision.HIGHEST)
    return (jnp.stack([residual_real, residual_imag]), adjoint.astype(jnp.bfloat16))

def reference(model_strip, screen_angle, facet_window, facet_shift, kernel_taps, plane_angle, u_cell, v_cell, w_plane, observed):

    def screen_strip(layer_index, facet_index):
        strip_values = model_strip[facet_index].astype(jnp.float32)
        phases = screen_angle[layer_index, facet_index].astype(jnp.float32)
        cosine = jnp.cos(phases)
        sine_part = jnp.sin(phases)
        return jnp.stack([strip_values[0] * cosine - strip_values[1] * sine_part, strip_values[0] * sine_part + strip_values[1] * cosine]).astype(jnp.bfloat16)

    def layer_grids(layer_index):

        def add_facet(running, facet_index):
            screened = screen_strip(layer_index, facet_index)
            contrib = forward(screened, facet_window[facet_index], facet_shift[facet_index])
            return (running + contrib.astype(jnp.float32), None)
        start = jnp.zeros((SUBGRIDS, SUB_ROWS, 2 * STRIP_COLS), jnp.float32)
        running, _ = lax.scan(add_facet, start, jnp.arange(FACETS, dtype=jnp.int32))
        return running
    grids = lax.map(layer_grids, jnp.arange(LAYERS, dtype=jnp.int32))
    angle_rows = jnp.repeat(plane_angle, SUBGRIDS, axis=0)

    def one_subgrid(inputs):
        subgrid, row_cells, column_cells, plane, observed_vis, angle_table = inputs
        return degrid(subgrid, row_cells, column_cells, plane, observed_vis, angle_table, kernel_taps)
    residual, adjoint = lax.map(one_subgrid, (grids.reshape(LAYERS * SUBGRIDS, SUB_ROWS, 2 * STRIP_COLS), u_cell.reshape(LAYERS * SUBGRIDS, VIS), v_cell.reshape(LAYERS * SUBGRIDS, VIS), w_plane.reshape(LAYERS * SUBGRIDS, VIS), observed.reshape(LAYERS * SUBGRIDS, 2, VIS), angle_rows))
    residual = residual.reshape(LAYERS, SUBGRIDS, 2, VIS)
    adjoint = adjoint.reshape(LAYERS, SUBGRIDS, SUB_ROWS, 2 * STRIP_COLS)

    def facet_gradient(facet_index):

        def add_layer(running, layer_index):
            term = backward(adjoint[layer_index], facet_window[facet_index], facet_shift[facet_index], screen_angle[layer_index, facet_index])
            rounded = lax.optimization_barrier(term.astype(jnp.bfloat16))
            return (running + rounded.astype(jnp.float32), None)
        start = jnp.zeros((2, STRIP_COLS, STRIP_LEN), jnp.float32)
        running, _ = lax.scan(add_layer, start, jnp.arange(LAYERS, dtype=jnp.int32))
        return running
    gradient = lax.map(facet_gradient, jnp.arange(FACETS, dtype=jnp.int32))
    return (residual, gradient)
```

```python
import functools
import math

import jax
import jax.numpy as jnp
import numpy as np
from jax import lax
from jax.experimental import pallas as pl
from jax.experimental.pallas import tpu as pltpu
from jax.sharding import PartitionSpec as P

MESH = pl.DeviceIdType.MESH
BACK_GAIN = 8.0
CHUNKS = 8


def _fit(values, degree):
    nodes = np.cos(np.pi * (np.arange(64) + 0.5) / 64)
    y = (nodes + 1.0) * 0.5 * np.pi**2
    cheb = np.polynomial.chebyshev.Chebyshev.fit(y, values(np.sqrt(y)), degree, domain=[0, np.pi**2])
    return [float(v) for v in cheb.convert(kind=np.polynomial.Polynomial).coef]


COS = _fit(np.cos, 8)
SIN = _fit(lambda x: np.sinc(x / np.pi), 7)


def cos_sin(x):
    y = x * x
    c = jnp.full_like(y, COS[-1])
    for v in COS[-2::-1]:
        c = c * y + v
    s = jnp.full_like(y, SIN[-1])
    for v in SIN[-2::-1]:
        s = s * y + v
    return c, s * x


def dft(length):
    k = np.arange(length)
    angles = 2.0 * np.pi * ((k[:, None] * k[None, :]) % length) / length
    scale = 1.0 / math.sqrt(length)
    return np.cos(angles) * scale, -np.sin(angles) * scale


def barrier_line(i, n):
    sem = pltpu.get_barrier_semaphore()

    @pl.when(i > 0)
    def _():
        pl.semaphore_signal(sem, inc=1, device_id={"layer": i - 1}, device_id_type=MESH)

    @pl.when(i < n - 1)
    def _():
        pl.semaphore_signal(sem, inc=1, device_id={"layer": i + 1}, device_id_type=MESH)

    peers = jnp.where(i > 0, 1, 0) + jnp.where(i < n - 1, 1, 0)
    pl.semaphore_wait(sem, peers)


def forward_kernel(n, x_ref, ang_ref, f1_ref, g_ref, tw_ref, fac_ref, out_ref, buf, send_sem, recv_sem, own_sem):
    i = lax.axis_index("layer")
    cq = x_ref.shape[0] // CHUNKS
    subgrids = g_ref.shape[0] // 2
    rows = f1_ref.shape[0] // 2
    barrier_line(i, n)
    own = pltpu.make_async_copy(x_ref, buf.at[i], own_sem)
    own.start()

    def copy(direction, s, q):
        step = 1 if direction == 0 else -1
        origin = jnp.clip(i - step * s, 0, n - 1)
        cols = pl.ds(q * cq, cq)
        src = x_ref.at[cols] if s == 0 else buf.at[origin, cols]
        return pltpu.make_async_remote_copy(
            src_ref=src,
            dst_ref=buf.at[origin, cols],
            send_sem=send_sem.at[direction, s, q],
            recv_sem=recv_sem.at[direction, s, q],
            device_id={"layer": jnp.clip(i + step, 0, n - 1)},
            device_id_type=MESH,
        )

    def sends(direction, s):
        if direction == 0:
            return (i - s >= 0) & (i < n - 1)
        return (i + s <= n - 1) & (i > 0)

    def gets(direction, s):
        return i - 1 - s >= 0 if direction == 0 else i + 1 + s <= n - 1

    def compute(q):
        twr, twi = tw_ref[0], tw_ref[1]
        facr, faci = fac_ref[0], fac_ref[1]
        for pair in range(cq // 2):
            halves = []
            for c in (2 * pair, 2 * pair + 1):
                col = q * cq + c
                xr = jnp.concatenate([buf[l, col, 0] for l in range(n)], axis=0).astype(jnp.float32)
                xi = jnp.concatenate([buf[l, col, 1] for l in range(n)], axis=0).astype(jnp.float32)
                cosine, sine = cos_sin(ang_ref[col].astype(jnp.float32))
                x = jnp.concatenate([xr * cosine - xi * sine, xr * sine + xi * cosine], axis=0)
                h = jnp.dot(f1_ref[...], x.astype(jnp.bfloat16), preferred_element_type=jnp.float32)
                hr, hi = h[:rows], h[rows:]
                halves.append(
                    jnp.concatenate([hr * twr - hi * twi, hr * twi + hi * twr], axis=1).astype(jnp.bfloat16)
                )
            both = jnp.concatenate(halves, axis=0)
            spec = lax.dot_general(
                g_ref[...], both, (((1,), (1,)), ((), ())), preferred_element_type=jnp.float32
            )
            sr, si = spec[:subgrids], spec[subgrids:]
            at = q * (cq // 2) + pair
            out_ref[0, at] = (sr * facr - si * faci).astype(jnp.bfloat16)
            out_ref[1, at] = (sr * faci + si * facr).astype(jnp.bfloat16)

    def body(t, carry):
        @pl.when(t < CHUNKS)
        def _():
            for d in range(2):
                @pl.when(sends(d, 0))
                def _():
                    copy(d, 0, t).start()

        for s in range(n - 1):
            q = t - 1 - s
            @pl.when((q >= 0) & (q < CHUNKS))
            def _():
                for d in range(2):
                    @pl.when(gets(d, s))
                    def _():
                        copy(d, s, q).wait_recv()
                        if s + 1 < n - 1:
                            @pl.when(sends(d, s + 1))
                            def _():
                                copy(d, s + 1, q).start()

        @pl.when(t >= n - 1)
        def _():
            compute(t - (n - 1))

        return carry

    own.wait()
    lax.fori_loop(0, CHUNKS + n - 1, body, 0)

    def drain(q, carry):
        for d in range(2):
            for s in range(n - 1):
                @pl.when(sends(d, s))
                def _():
                    copy(d, s, q).wait_send()
        return carry

    lax.fori_loop(0, CHUNKS, drain, 0)


def backward_kernel(n, a_ref, ang_ref, g_ref, f2_ref, tw_ref, fac_ref, out_ref, term, sbuf, rbuf, send_sem, recv_sem):
    i = lax.axis_index("layer")
    cols = ang_ref.shape[0]
    cq = cols // CHUNKS
    fine = g_ref.shape[0] // 2
    rows = ang_ref.shape[1]
    part = rows // n
    barrier_line(i, n)

    def copy(direction, j, q):
        where = pl.ds(q * cq, cq)
        step = 1 if direction == 0 else -1
        return pltpu.make_async_remote_copy(
            src_ref=sbuf.at[direction, j, where],
            dst_ref=rbuf.at[direction, j, where],
            send_sem=send_sem.at[direction, j, q],
            recv_sem=recv_sem.at[direction, j, q],
            device_id={"layer": jnp.clip(i + step, 0, n - 1)},
            device_id_type=MESH,
        )

    def behind(direction):
        return i > 0 if direction == 0 else i < n - 1

    def compute(q):
        twr, twi = tw_ref[0], tw_ref[1]
        facr, faci = fac_ref[0], fac_ref[1]
        for pair in range(cq // 2):
            at = q * (cq // 2) + pair
            ar = a_ref[0, at].astype(jnp.float32)
            ai = a_ref[1, at].astype(jnp.float32)
            b = jnp.concatenate([ar * facr + ai * faci, ai * facr - ar * faci], axis=0).astype(jnp.bfloat16)
            h = jnp.dot(g_ref[...], b, preferred_element_type=jnp.float32)
            hr, hi = h[:fine], h[fine:]
            mixed = jnp.concatenate([hr * twr + hi * twi, hi * twr - hr * twi], axis=1).astype(jnp.bfloat16)
            image = lax.dot_general(
                f2_ref[...], mixed, (((1,), (1,)), ((), ())), preferred_element_type=jnp.float32
            )
            for c in range(2):
                col = q * cq + 2 * pair + c
                ir = image[2 * c * rows : (2 * c + 1) * rows]
                ii = image[(2 * c + 1) * rows : (2 * c + 2) * rows]
                cosine, sine = cos_sin(ang_ref[col].astype(jnp.float32))
                tr = (BACK_GAIN * (ir * cosine + ii * sine)).astype(jnp.bfloat16)
                ti = (BACK_GAIN * (ii * cosine - ir * sine)).astype(jnp.bfloat16)
                for l in range(n):
                    term[l, col, 0] = tr[l * part : (l + 1) * part]
                    term[l, col, 1] = ti[l * part : (l + 1) * part]

    def relay(direction, j, q):
        where = pl.ds(q * cq, cq)

        @pl.when(behind(direction))
        def _():
            copy(direction, j, q).wait_recv()
            total = term[j, where].astype(jnp.float32) + rbuf[direction, j, where].astype(jnp.float32)
            sbuf[direction, j, where] = total.astype(jnp.bfloat16)

        @pl.when(jnp.logical_not(behind(direction)))
        def _():
            sbuf[direction, j, where] = term[j, where]

        copy(direction, j, q).start()

    def body(t, carry):
        @pl.when(t < CHUNKS)
        def _():
            compute(t)

        for direction in range(2):
            q = t - i if direction == 0 else t - (n - 1 - i)

            @pl.when((q >= 0) & (q < CHUNKS))
            def _():
                for d in range(n - 1, 0, -1):
                    j = i + d if direction == 0 else i - d

                    @pl.when((j < n) & (j >= 0))
                    def _():
                        relay(direction, j, q)

        last = t - (n - 1)

        @pl.when(last >= 0)
        def _():
            where = pl.ds(last * cq, cq)
            out_ref[where] = term[i, where].astype(jnp.float32)
            for direction in range(2):
                @pl.when(behind(direction))
                def _():
                    copy(direction, i, last).wait_recv()
                    out_ref[where] += rbuf[direction, i, where].astype(jnp.float32)

        return carry

    lax.fori_loop(0, CHUNKS + n - 1, body, 0)

    def drain(q, carry):
        for direction in range(2):
            for d in range(1, n):
                j = i + d if direction == 0 else i - d

                @pl.when((j < n) & (j >= 0))
                def _():
                    copy(direction, j, q).wait_send()
        return carry

    lax.fori_loop(0, CHUNKS, drain, 0)


def facet_factor(window, shift_cells, subgrids):
    length = window.shape[0]
    positions = jnp.arange(length, dtype=jnp.int32)
    turn_count = positions * shift_cells % length
    angles = 2.0 * math.pi / length * turn_count.astype(jnp.float32)
    both = jnp.stack([window * jnp.cos(angles), -window * jnp.sin(angles)]).reshape(2, subgrids, -1)
    return jnp.concatenate([both, both], axis=2)


def spread(cells, length, taps):
    count = taps.shape[0]
    lanes = jnp.arange(length, dtype=jnp.int32)
    offset = (lanes - cells[..., None] + (count // 2 + length)) % length
    out = jnp.zeros(offset.shape, jnp.float32)
    for t in range(count):
        out = out + jnp.where(offset == t, taps[t], 0.0)
    return out


def middle(grids, u, v, plane, observed, angle, taps, rows, cols):
    row_weights = spread(u, rows, taps)
    column_weights = spread(v, cols, taps).astype(jnp.bfloat16)
    picked = jnp.einsum("sjc,sck->sjk", column_weights, grids.astype(jnp.bfloat16), preferred_element_type=jnp.float32)
    model_real = jnp.sum(picked[..., :rows] * row_weights, axis=2)
    model_imag = jnp.sum(picked[..., rows:] * row_weights, axis=2)
    pick = plane[..., None] == jnp.arange(angle.shape[0], dtype=jnp.int32)
    cosine = jnp.sum(jnp.where(pick, jnp.cos(angle), 0.0), axis=2)
    sine = jnp.sum(jnp.where(pick, jnp.sin(angle), 0.0), axis=2)
    res_real = observed[:, 0] - (model_real * cosine - model_imag * sine)
    res_imag = observed[:, 1] - (model_real * sine + model_imag * cosine)
    w_real = res_real * cosine + res_imag * sine
    w_imag = res_imag * cosine - res_real * sine
    spread_rows = jnp.concatenate(
        [w_real[..., None] * row_weights, w_imag[..., None] * row_weights], axis=2
    ).astype(jnp.bfloat16)
    adjoint = jnp.einsum("sjc,sjk->sck", column_weights, spread_rows, preferred_element_type=jnp.float32)
    return jnp.stack([res_real, res_imag], axis=1), adjoint.astype(jnp.bfloat16)


def local(n, nf, model_strip, screen_angle, facet_window, facet_shift, kernel_taps, plane_angle, u_cell, v_cell, w_plane, observed):
    _, _, cols, length = screen_angle.shape
    per = u_cell.shape[1]
    subgrids = per * nf
    rows = length // subgrids
    block = rows // n
    vmem = pl.BlockSpec(memory_space=pltpu.VMEM)
    fr, fi = dft(rows)
    gr, gi = dft(subgrids)
    turn = 2.0 * np.pi * (np.arange(rows)[:, None] * np.arange(subgrids)[None, :] % length) / length
    twist = np.stack([np.cos(turn), -np.sin(turn)]).astype(np.float32)
    bf = lambda a: jnp.asarray(a.astype(np.float32)).astype(jnp.bfloat16)
    f1 = bf(np.block([[fr, -fi], [fi, fr]]))
    g1 = bf(np.block([[gr, -gi], [gi, gr]]))
    g2 = bf(np.block([[gr.T, gi.T], [-gi.T, gr.T]]))
    zero = np.zeros_like(fr)
    f2 = bf(
        np.block(
            [
                [fr.T, zero, fi.T, zero],
                [-fi.T, zero, fr.T, zero],
                [zero, fr.T, zero, fi.T],
                [zero, -fi.T, zero, fr.T],
            ]
        )
    )
    tw2 = np.ascontiguousarray(np.tile(np.swapaxes(twist, 1, 2), (1, 1, 2)))
    factor = facet_factor(facet_window[0], facet_shift[0], subgrids)
    x = model_strip[0].reshape(2, cols, block, subgrids).transpose(1, 0, 2, 3)
    angle = screen_angle[0, 0].reshape(cols, rows, subgrids)
    contrib = pl.pallas_call(
        functools.partial(forward_kernel, n),
        out_shape=jax.ShapeDtypeStruct((2, cols // 2, subgrids, 2 * rows), jnp.bfloat16),
        in_specs=[vmem] * 6,
        out_specs=vmem,
        scratch_shapes=[
            pltpu.VMEM((n, cols, 2, block, subgrids), jnp.bfloat16),
            pltpu.SemaphoreType.DMA((2, n - 1, CHUNKS)),
            pltpu.SemaphoreType.DMA((2, n - 1, CHUNKS)),
            pltpu.SemaphoreType.DMA,
        ],
        compiler_params=pltpu.CompilerParams(collective_id=0, has_side_effects=True),
        name="gather_forward",
    )(x, angle, f1, g1, jnp.asarray(twist), factor)
    parts = contrib.reshape(2, cols // 2, nf, per, 2 * rows)
    received = lax.all_to_all(parts, "facet", split_axis=2, concat_axis=2, tiled=True)
    grids = jnp.sum(received.astype(jnp.float32), axis=2)
    grids = grids.reshape(2, cols // 2, per, 2, rows).transpose(2, 1, 3, 0, 4).reshape(per, cols, 2 * rows)
    residual, adjoint = middle(
        grids, u_cell[0], v_cell[0], w_plane[0], observed[0], plane_angle[0], kernel_taps, rows, cols
    )
    adjoint = adjoint.reshape(per, cols // 2, 2, 2, rows).transpose(3, 1, 0, 2, 4).reshape(2, cols // 2, per, 2 * rows)
    every = lax.all_gather(adjoint, "facet", axis=2, tiled=True)
    gradient = pl.pallas_call(
        functools.partial(backward_kernel, n),
        out_shape=jax.ShapeDtypeStruct((cols, 2, block, subgrids), jnp.float32),
        in_specs=[vmem] * 6,
        out_specs=vmem,
        scratch_shapes=[
            pltpu.VMEM((n, cols, 2, block, subgrids), jnp.bfloat16),
            pltpu.VMEM((2, n, cols, 2, block, subgrids), jnp.bfloat16),
            pltpu.VMEM((2, n, cols, 2, block, subgrids), jnp.bfloat16),
            pltpu.SemaphoreType.DMA((2, n, CHUNKS)),
            pltpu.SemaphoreType.DMA((2, n, CHUNKS)),
        ],
        compiler_params=pltpu.CompilerParams(collective_id=1, has_side_effects=True),
        name="backward_scatter",
    )(every, angle, g2, f2, jnp.asarray(tw2), factor)
    gradient = gradient.transpose(1, 0, 2, 3).reshape(1, 2, cols, block * subgrids)
    return (residual[None], gradient)


def solution(mesh):
    return jax.shard_map(
        functools.partial(local, mesh.shape["layer"], mesh.shape["facet"]),
        mesh=mesh,
        in_specs=(
            P("facet", None, None, "layer"),
            P("layer", "facet", None, None),
            P("facet", None),
            P("facet"),
            P(),
            P("layer", None),
            P("layer", "facet", None),
            P("layer", "facet", None),
            P("layer", "facet", None),
            P("layer", "facet", None, None),
        ),
        out_specs=(P("layer", "facet", None, None), P("facet", None, None, "layer")),
        check_vma=False,
    )
```

```python
import functools
import math

import jax
import jax.numpy as jnp
import numpy as np
from jax import lax
from jax.experimental import pallas as pl
from jax.experimental.pallas import tpu as pltpu
from jax.sharding import PartitionSpec as P

MESH = pl.DeviceIdType.MESH
BACK_GAIN = 8.0
CHUNKS = 8


def _fit(values, degree):
    nodes = np.cos(np.pi * (np.arange(64) + 0.5) / 64)
    y = (nodes + 1.0) * 0.5 * np.pi**2
    cheb = np.polynomial.chebyshev.Chebyshev.fit(y, values(np.sqrt(y)), degree, domain=[0, np.pi**2])
    return [float(v) for v in cheb.convert(kind=np.polynomial.Polynomial).coef]


COS = _fit(np.cos, 8)
SIN = _fit(lambda x: np.sinc(x / np.pi), 7)


def cos_sin(x):
    y = x * x
    c = jnp.full_like(y, COS[-1])
    for v in COS[-2::-1]:
        c = c * y + v
    s = jnp.full_like(y, SIN[-1])
    for v in SIN[-2::-1]:
        s = s * y + v
    return c, s * x


def dft(length):
    k = np.arange(length)
    angles = 2.0 * np.pi * ((k[:, None] * k[None, :]) % length) / length
    scale = 1.0 / math.sqrt(length)
    return np.cos(angles) * scale, -np.sin(angles) * scale


def barrier_line(i, n):
    sem = pltpu.get_barrier_semaphore()

    @pl.when(i > 0)
    def _():
        pl.semaphore_signal(sem, inc=1, device_id={"layer": i - 1}, device_id_type=MESH)

    @pl.when(i < n - 1)
    def _():
        pl.semaphore_signal(sem, inc=1, device_id={"layer": i + 1}, device_id_type=MESH)

    peers = jnp.where(i > 0, 1, 0) + jnp.where(i < n - 1, 1, 0)
    pl.semaphore_wait(sem, peers)


def forward_kernel(n, x_ref, ang_ref, f1_ref, g_ref, tw_ref, fac_ref, out_ref, buf, send_sem, recv_sem, own_sem):
    i = lax.axis_index("layer")
    cq = x_ref.shape[0] // CHUNKS
    subgrids = g_ref.shape[0] // 2
    rows = f1_ref.shape[0] // 2
    barrier_line(i, n)
    own = pltpu.make_async_copy(x_ref, buf.at[i], own_sem)
    own.start()

    def copy(direction, s, q):
        step = 1 if direction == 0 else -1
        origin = jnp.clip(i - step * s, 0, n - 1)
        cols = pl.ds(q * cq, cq)
        src = x_ref.at[cols] if s == 0 else buf.at[origin, cols]
        return pltpu.make_async_remote_copy(
            src_ref=src,
            dst_ref=buf.at[origin, cols],
            send_sem=send_sem.at[direction, s, q],
            recv_sem=recv_sem.at[direction, s, q],
            device_id={"layer": jnp.clip(i + step, 0, n - 1)},
            device_id_type=MESH,
        )

    def sends(direction, s):
        if direction == 0:
            return (i - s >= 0) & (i < n - 1)
        return (i + s <= n - 1) & (i > 0)

    def gets(direction, s):
        return i - 1 - s >= 0 if direction == 0 else i + 1 + s <= n - 1

    def compute(q):
        twr, twi = tw_ref[0], tw_ref[1]
        facr, faci = fac_ref[0], fac_ref[1]
        for pair in range(cq // 2):
            halves = []
            for c in (2 * pair, 2 * pair + 1):
                col = q * cq + c
                xr = jnp.concatenate([buf[l, col, 0] for l in range(n)], axis=0).astype(jnp.float32)
                xi = jnp.concatenate([buf[l, col, 1] for l in range(n)], axis=0).astype(jnp.float32)
                cosine, sine = cos_sin(ang_ref[col].astype(jnp.float32))
                x = jnp.concatenate([xr * cosine - xi * sine, xr * sine + xi * cosine], axis=0)
                h = jnp.dot(f1_ref[...], x.astype(jnp.bfloat16), preferred_element_type=jnp.float32)
                hr, hi = h[:rows], h[rows:]
                halves.append(
                    jnp.concatenate([hr * twr - hi * twi, hr * twi + hi * twr], axis=1).astype(jnp.bfloat16)
                )
            both = jnp.concatenate(halves, axis=0)
            spec = lax.dot_general(
                g_ref[...], both, (((1,), (1,)), ((), ())), preferred_element_type=jnp.float32
            )
            sr, si = spec[:subgrids], spec[subgrids:]
            at = q * (cq // 2) + pair
            out_ref[0, at] = (sr * facr - si * faci).astype(jnp.bfloat16)
            out_ref[1, at] = (sr * faci + si * facr).astype(jnp.bfloat16)

    def body(t, carry):
        @pl.when(t < CHUNKS)
        def _():
            for d in range(2):
                @pl.when(sends(d, 0))
                def _():
                    copy(d, 0, t).start()

        for s in range(n - 1):
            q = t - 1 - s
            @pl.when((q >= 0) & (q < CHUNKS))
            def _():
                for d in range(2):
                    @pl.when(gets(d, s))
                    def _():
                        copy(d, s, q).wait_recv()
                        if s + 1 < n - 1:
                            @pl.when(sends(d, s + 1))
                            def _():
                                copy(d, s + 1, q).start()

        @pl.when(t >= n - 1)
        def _():
            compute(t - (n - 1))

        return carry

    own.wait()
    lax.fori_loop(0, CHUNKS + n - 1, body, 0)

    def drain(q, carry):
        for d in range(2):
            for s in range(n - 1):
                @pl.when(sends(d, s))
                def _():
                    copy(d, s, q).wait_send()
        return carry

    lax.fori_loop(0, CHUNKS, drain, 0)


def backward_kernel(n, a_ref, ang_ref, g_ref, f2_ref, tw_ref, fac_ref, out_ref, term, sbuf, rbuf, send_sem, recv_sem):
    i = lax.axis_index("layer")
    cols = ang_ref.shape[0]
    cq = cols // CHUNKS
    fine = g_ref.shape[0] // 2
    rows = ang_ref.shape[1]
    part = rows // n
    barrier_line(i, n)

    def copy(direction, j, q):
        where = pl.ds(q * cq, cq)
        step = 1 if direction == 0 else -1
        return pltpu.make_async_remote_copy(
            src_ref=sbuf.at[direction, j, where],
            dst_ref=rbuf.at[direction, j, where],
            send_sem=send_sem.at[direction, j, q],
            recv_sem=recv_sem.at[direction, j, q],
            device_id={"layer": jnp.clip(i + step, 0, n - 1)},
            device_id_type=MESH,
        )

    def behind(direction):
        return i > 0 if direction == 0 else i < n - 1

    def compute(q):
        twr, twi = tw_ref[0], tw_ref[1]
        facr, faci = fac_ref[0], fac_ref[1]
        for pair in range(cq // 2):
            at = q * (cq // 2) + pair
            ar = a_ref[0, at].astype(jnp.float32)
            ai = a_ref[1, at].astype(jnp.float32)
            b = jnp.concatenate([ar * facr + ai * faci, ai * facr - ar * faci], axis=0).astype(jnp.bfloat16)
            h = jnp.dot(g_ref[...], b, preferred_element_type=jnp.float32)
            hr, hi = h[:fine], h[fine:]
            mixed = jnp.concatenate([hr * twr + hi * twi, hi * twr - hr * twi], axis=1).astype(jnp.bfloat16)
            image = lax.dot_general(
                f2_ref[...], mixed, (((1,), (1,)), ((), ())), preferred_element_type=jnp.float32
            )
            for c in range(2):
                col = q * cq + 2 * pair + c
                ir = image[2 * c * rows : (2 * c + 1) * rows]
                ii = image[(2 * c + 1) * rows : (2 * c + 2) * rows]
                cosine, sine = cos_sin(ang_ref[col].astype(jnp.float32))
                tr = (BACK_GAIN * (ir * cosine + ii * sine)).astype(jnp.bfloat16)
                ti = (BACK_GAIN * (ii * cosine - ir * sine)).astype(jnp.bfloat16)
                for l in range(n):
                    term[l, col, 0] = tr[l * part : (l + 1) * part]
                    term[l, col, 1] = ti[l * part : (l + 1) * part]

    def relay(direction, j, q):
        where = pl.ds(q * cq, cq)

        @pl.when(behind(direction))
        def _():
            copy(direction, j, q).wait_recv()
            total = term[j, where].astype(jnp.float32) + rbuf[direction, j, where].astype(jnp.float32)
            sbuf[direction, j, where] = total.astype(jnp.bfloat16)

        @pl.when(jnp.logical_not(behind(direction)))
        def _():
            sbuf[direction, j, where] = term[j, where]

        copy(direction, j, q).start()

    def body(t, carry):
        @pl.when(t < CHUNKS)
        def _():
            compute(t)

        for direction in range(2):
            q = t - i if direction == 0 else t - (n - 1 - i)

            @pl.when((q >= 0) & (q < CHUNKS))
            def _():
                for d in range(n - 1, 0, -1):
                    j = i + d if direction == 0 else i - d

                    @pl.when((j < n) & (j >= 0))
                    def _():
                        relay(direction, j, q)

        last = t - (n - 1)

        @pl.when(last >= 0)
        def _():
            where = pl.ds(last * cq, cq)
            out_ref[where] = term[i, where].astype(jnp.float32)
            for direction in range(2):
                @pl.when(behind(direction))
                def _():
                    copy(direction, i, last).wait_recv()
                    out_ref[where] += rbuf[direction, i, where].astype(jnp.float32)

        return carry

    lax.fori_loop(0, CHUNKS + n - 1, body, 0)

    def drain(q, carry):
        for direction in range(2):
            for d in range(1, n):
                j = i + d if direction == 0 else i - d

                @pl.when((j < n) & (j >= 0))
                def _():
                    copy(direction, j, q).wait_send()
        return carry

    lax.fori_loop(0, CHUNKS, drain, 0)


def facet_factor(window, shift_cells, subgrids):
    length = window.shape[0]
    positions = jnp.arange(length, dtype=jnp.int32)
    turn_count = positions * shift_cells % length
    angles = 2.0 * math.pi / length * turn_count.astype(jnp.float32)
    both = jnp.stack([window * jnp.cos(angles), -window * jnp.sin(angles)]).reshape(2, subgrids, -1)
    return jnp.concatenate([both, both], axis=2)


def spread(cells, length, taps):
    count = taps.shape[0]
    lanes = jnp.arange(length, dtype=jnp.int32)
    offset = (lanes - cells[..., None] + (count // 2 + length)) % length
    out = jnp.zeros(offset.shape, jnp.float32)
    for t in range(count):
        out = out + jnp.where(offset == t, taps[t], 0.0)
    return out


def middle(grids, u, v, plane, observed, angle, taps, rows, cols):
    row_weights = spread(u, rows, taps)
    column_weights = spread(v, cols, taps).astype(jnp.bfloat16)
    picked = jnp.einsum("sjc,sck->sjk", column_weights, grids.astype(jnp.bfloat16), preferred_element_type=jnp.float32)
    model_real = jnp.sum(picked[..., :rows] * row_weights, axis=2)
    model_imag = jnp.sum(picked[..., rows:] * row_weights, axis=2)
    pick = plane[..., None] == jnp.arange(angle.shape[0], dtype=jnp.int32)
    cosine = jnp.sum(jnp.where(pick, jnp.cos(angle), 0.0), axis=2)
    sine = jnp.sum(jnp.where(pick, jnp.sin(angle), 0.0), axis=2)
    res_real = observed[:, 0] - (model_real * cosine - model_imag * sine)
    res_imag = observed[:, 1] - (model_real * sine + model_imag * cosine)
    w_real = res_real * cosine + res_imag * sine
    w_imag = res_imag * cosine - res_real * sine
    spread_rows = jnp.concatenate(
        [w_real[..., None] * row_weights, w_imag[..., None] * row_weights], axis=2
    ).astype(jnp.bfloat16)
    adjoint = jnp.einsum("sjc,sjk->sck", column_weights, spread_rows, preferred_element_type=jnp.float32)
    return jnp.stack([res_real, res_imag], axis=1), adjoint.astype(jnp.bfloat16)


def middle_kernel(
    contrib_ref, u_ref, v_ref, plane_ref, obs_ref, taps_ref, table_ref, res_ref, out_ref,
    r0, acc0, r1, acc1, r2, fin, adj, phase, s0, d0, s1, d1, s2, d2, sg, dg,
):
    pairs = contrib_ref.shape[1]
    per, vis = u_ref.shape
    rows = contrib_ref.shape[3] // 2
    cols = 2 * pairs
    f = lax.axis_index("facet")
    core = lax.rem(f, 2)
    chip = lax.div(f, 2)
    bits = (lax.rem(chip, 2), lax.div(chip, 2))

    def flip(b):
        return f + (1 - 2 * bits[b]) * (2 * (1 + b))

    other = f + 1 - 2 * core
    barrier = pltpu.get_barrier_semaphore()
    for peer in (other, flip(0), flip(1)):
        pl.semaphore_signal(barrier, inc=1, device_id={"facet": peer}, device_id_type=MESH)
    pl.semaphore_wait(barrier, 3)

    def rows_of(device):
        return pl.ds(pl.multiple_of(device * per, per), per)

    def compose(p, along, across):
        return along + 2 * across if p == 0 else across + 2 * along

    def remote(src, dst, send, recv, device):
        return pltpu.make_async_remote_copy(
            src_ref=src, dst_ref=dst, send_sem=send, recv_sem=recv,
            device_id={"facet": device}, device_id_type=MESH,
        )

    def stage0(p, h):
        return remote(
            contrib_ref.at[p, :, rows_of(2 * h + 1 - core)], r0.at[p, h], s0.at[p, h], d0.at[p, h], other
        )

    def stage1(p, k):
        return remote(acc0.at[p, compose(p, 1 - bits[p], k)], r1.at[p, k], s1.at[p, k], d1.at[p, k], flip(p))

    def stage2(p):
        return remote(acc1.at[p, 1 - bits[1 - p]], r2.at[p], s2.at[p], d2.at[p], flip(1 - p))

    def add0(p, h):
        stage0(p, h).wait_recv()
        mine = contrib_ref[p, :, rows_of(2 * h + core)].astype(jnp.float32)
        acc0[p, h] = (mine + r0[p, h].astype(jnp.float32)).astype(jnp.bfloat16)

    order = [(a, k, p) for a in (1, 0) for k in range(2) for p in range(2)]
    for a, k, p in order:
        stage0(p, compose(p, 1 - bits[p] if a else bits[p], k)).start()
    for k in range(2):
        for p in range(2):
            add0(p, compose(p, 1 - bits[p], k))
            stage1(p, k).start()
    for k in range(2):
        for p in range(2):
            add0(p, compose(p, bits[p], k))

    plane = plane_ref[...]
    cosine = jnp.zeros(plane.shape, jnp.float32)
    sine = jnp.zeros(plane.shape, jnp.float32)
    for k in range(table_ref.shape[1]):
        hit = plane == k
        cosine = jnp.where(hit, table_ref[0, k], cosine)
        sine = jnp.where(hit, table_ref[1, k], sine)
    phase[0] = cosine
    phase[1] = sine

    for k in range(2):
        for p in range(2):
            stage1(p, k).wait_recv()
            total = acc0[p, compose(p, bits[p], k)].astype(jnp.float32) + r1[p, k].astype(jnp.float32)
            acc1[p, k] = total.astype(jnp.bfloat16)
    for p in range(2):
        stage2(p).start()
    for p in range(2):
        stage2(p).wait_recv()
        for t in range(pairs):
            total = acc1[p, bits[1 - p], t].astype(jnp.float32) + r2[p, t].astype(jnp.float32)
            fin[p, pl.ds(t, per, stride=pairs), :] = total

    def weights(cells, position, length):
        count = taps_ref.shape[0]
        offset = position - cells + count // 2
        offset = jnp.where(offset < 0, offset + length, jnp.where(offset >= length, offset - length, offset))
        out = jnp.zeros(offset.shape, jnp.float32)
        for t in range(count):
            out = jnp.where(offset == t, taps_ref[t], out)
        return out

    def one(s, carry):
        at = pl.ds(s, 1)
        where = pl.ds(pl.multiple_of(s * pairs, pairs), pairs)
        row = lax.broadcasted_iota(jnp.int32, (rows, vis), 0)
        half = lax.broadcasted_iota(jnp.int32, (pairs, vis), 0)
        col = jnp.concatenate([2 * half, 2 * half + 1], axis=0)
        row_weights = weights(u_ref[at, :], row, rows)
        column_weights = weights(v_ref[at, :], col, cols).astype(jnp.bfloat16)
        real, imag = fin[0, where, :], fin[1, where, :]
        grid = jnp.concatenate(
            [
                jnp.concatenate([real[:, :rows], imag[:, :rows]], axis=1),
                jnp.concatenate([real[:, rows:], imag[:, rows:]], axis=1),
            ],
            axis=0,
        )
        picked = lax.dot_general(
            grid.astype(jnp.bfloat16), column_weights, (((0,), (0,)), ((), ())),
            preferred_element_type=jnp.float32,
        )
        model_real = jnp.sum(picked[:rows] * row_weights, axis=0, keepdims=True)
        model_imag = jnp.sum(picked[rows:] * row_weights, axis=0, keepdims=True)
        cosine, sine = phase[0, at, :], phase[1, at, :]
        res_real = obs_ref[s, 0:1, :] - (model_real * cosine - model_imag * sine)
        res_imag = obs_ref[s, 1:2, :] - (model_real * sine + model_imag * cosine)
        res_ref[s, 0:1, :] = res_real
        res_ref[s, 1:2, :] = res_imag
        w_real = res_real * cosine + res_imag * sine
        w_imag = res_imag * cosine - res_real * sine
        spread_rows = jnp.concatenate([row_weights * w_real, row_weights * w_imag], axis=0).astype(jnp.bfloat16)
        back = lax.dot_general(
            column_weights, spread_rows, (((1,), (1,)), ((), ())), preferred_element_type=jnp.float32
        )
        adj[0, where, :] = jnp.concatenate([back[:pairs, :rows], back[pairs:, :rows]], axis=1)
        adj[1, where, :] = jnp.concatenate([back[:pairs, rows:], back[pairs:, rows:]], axis=1)
        return carry

    lax.fori_loop(0, per, one, 0)

    def gather(step, p, device, peer):
        block = out_ref.at[p, :, rows_of(device)]
        return remote(block, block, sg.at[step, p, device], dg.at[p, device], peer)

    def far(p, a, k):
        along = 1 - bits[p] if a else bits[p]
        across = 1 - bits[1 - p] if k else bits[1 - p]
        return 2 * compose(p, along, across) + core

    for p in range(2):
        for t in range(pairs):
            out_ref[p, t, rows_of(f)] = adj[p, pl.ds(t, per, stride=pairs), :].astype(jnp.bfloat16)
        gather(0, p, f, flip(1 - p)).start()
        gather(1, p, f, flip(p)).start()
        gather(2, p, f, other).start()
    for p in range(2):
        block = far(p, 0, 1)
        gather(0, p, block, flip(1 - p)).wait_recv()
        gather(1, p, block, flip(p)).start()
        gather(2, p, block, other).start()
    for k in range(2):
        for p in range(2):
            block = far(p, 1, k)
            gather(1, p, block, flip(p)).wait_recv()
            gather(2, p, block, other).start()
    for p in range(2):
        for h in range(4):
            gather(2, p, 2 * h + 1 - core, other).wait_recv()
    for p in range(2):
        for h in range(4):
            stage0(p, h).wait_send()
            gather(2, p, 2 * h + core, other).wait_send()
        for k in range(2):
            stage1(p, k).wait_send()
            gather(1, p, far(p, 0, k), flip(p)).wait_send()
        stage2(p).wait_send()
        gather(0, p, f, flip(1 - p)).wait_send()


def fused_middle(contrib, u, v, plane, observed, taps, table):
    _, pairs, subgrids, lanes = contrib.shape
    per, vis = u.shape
    vmem = pl.BlockSpec(memory_space=pltpu.VMEM)
    smem = pl.BlockSpec(memory_space=pltpu.SMEM)
    block = (pairs, per, lanes)
    wire = lambda *lead: pltpu.VMEM((*lead, *block), jnp.bfloat16)
    dma = lambda *shape: pltpu.SemaphoreType.DMA(shape)
    return pl.pallas_call(
        middle_kernel,
        out_shape=(
            jax.ShapeDtypeStruct((per, 2, vis), jnp.float32),
            jax.ShapeDtypeStruct(contrib.shape, jnp.bfloat16),
        ),
        in_specs=[vmem] * 5 + [smem] * 2,
        out_specs=(vmem, vmem),
        scratch_shapes=[
            wire(2, 4), wire(2, 4), wire(2, 2), wire(2, 2), wire(2),
            pltpu.VMEM((2, per * pairs, lanes), jnp.float32),
            pltpu.VMEM((2, per * pairs, lanes), jnp.float32),
            pltpu.VMEM((2, per, vis), jnp.float32),
            dma(2, 4), dma(2, 4), dma(2, 2), dma(2, 2), dma(2), dma(2), dma(3, 2, 8), dma(2, 8),
        ],
        compiler_params=pltpu.CompilerParams(collective_id=2, has_side_effects=True),
        name="degrid_exchange",
    )(contrib, u, v, plane, observed, taps, table)


def local(n, nf, model_strip, screen_angle, facet_window, facet_shift, kernel_taps, plane_angle, u_cell, v_cell, w_plane, observed):
    _, _, cols, length = screen_angle.shape
    per = u_cell.shape[1]
    subgrids = per * nf
    rows = length // subgrids
    block = rows // n
    vmem = pl.BlockSpec(memory_space=pltpu.VMEM)
    fr, fi = dft(rows)
    gr, gi = dft(subgrids)
    turn = 2.0 * np.pi * (np.arange(rows)[:, None] * np.arange(subgrids)[None, :] % length) / length
    twist = np.stack([np.cos(turn), -np.sin(turn)]).astype(np.float32)
    bf = lambda a: jnp.asarray(a.astype(np.float32)).astype(jnp.bfloat16)
    f1 = bf(np.block([[fr, -fi], [fi, fr]]))
    g1 = bf(np.block([[gr, -gi], [gi, gr]]))
    g2 = bf(np.block([[gr.T, gi.T], [-gi.T, gr.T]]))
    zero = np.zeros_like(fr)
    f2 = bf(
        np.block(
            [
                [fr.T, zero, fi.T, zero],
                [-fi.T, zero, fr.T, zero],
                [zero, fr.T, zero, fi.T],
                [zero, -fi.T, zero, fr.T],
            ]
        )
    )
    tw2 = np.ascontiguousarray(np.tile(np.swapaxes(twist, 1, 2), (1, 1, 2)))
    factor = facet_factor(facet_window[0], facet_shift[0], subgrids)
    x = model_strip[0].reshape(2, cols, block, subgrids).transpose(1, 0, 2, 3)
    angle = screen_angle[0, 0].reshape(cols, rows, subgrids)
    contrib = pl.pallas_call(
        functools.partial(forward_kernel, n),
        out_shape=jax.ShapeDtypeStruct((2, cols // 2, subgrids, 2 * rows), jnp.bfloat16),
        in_specs=[vmem] * 6,
        out_specs=vmem,
        scratch_shapes=[
            pltpu.VMEM((n, cols, 2, block, subgrids), jnp.bfloat16),
            pltpu.SemaphoreType.DMA((2, n - 1, CHUNKS)),
            pltpu.SemaphoreType.DMA((2, n - 1, CHUNKS)),
            pltpu.SemaphoreType.DMA,
        ],
        compiler_params=pltpu.CompilerParams(collective_id=0, has_side_effects=True),
        name="gather_forward",
    )(x, angle, f1, g1, jnp.asarray(twist), factor)
    if nf == 8 and per % 16 == 0:
        table = jnp.stack([jnp.cos(plane_angle[0]), jnp.sin(plane_angle[0])])
        residual, every = fused_middle(
            contrib, u_cell[0], v_cell[0], w_plane[0], observed[0], kernel_taps, table
        )
    else:
        parts = contrib.reshape(2, cols // 2, nf, per, 2 * rows)
        received = lax.all_to_all(parts, "facet", split_axis=2, concat_axis=2, tiled=True)
        grids = jnp.sum(received.astype(jnp.float32), axis=2)
        grids = grids.reshape(2, cols // 2, per, 2, rows).transpose(2, 1, 3, 0, 4).reshape(per, cols, 2 * rows)
        residual, adjoint = middle(
            grids, u_cell[0], v_cell[0], w_plane[0], observed[0], plane_angle[0], kernel_taps, rows, cols
        )
        adjoint = adjoint.reshape(per, cols // 2, 2, 2, rows).transpose(3, 1, 0, 2, 4).reshape(2, cols // 2, per, 2 * rows)
        every = lax.all_gather(adjoint, "facet", axis=2, tiled=True)
    gradient = pl.pallas_call(
        functools.partial(backward_kernel, n),
        out_shape=jax.ShapeDtypeStruct((cols, 2, block, subgrids), jnp.float32),
        in_specs=[vmem] * 6,
        out_specs=vmem,
        scratch_shapes=[
            pltpu.VMEM((n, cols, 2, block, subgrids), jnp.bfloat16),
            pltpu.VMEM((2, n, cols, 2, block, subgrids), jnp.bfloat16),
            pltpu.VMEM((2, n, cols, 2, block, subgrids), jnp.bfloat16),
            pltpu.SemaphoreType.DMA((2, n, CHUNKS)),
            pltpu.SemaphoreType.DMA((2, n, CHUNKS)),
        ],
        compiler_params=pltpu.CompilerParams(collective_id=1, has_side_effects=True),
        name="backward_scatter",
    )(every, angle, g2, f2, jnp.asarray(tw2), factor)
    gradient = gradient.transpose(1, 0, 2, 3).reshape(1, 2, cols, block * subgrids)
    return (residual[None], gradient)


def solution(mesh):
    return jax.shard_map(
        functools.partial(local, mesh.shape["layer"], mesh.shape["facet"]),
        mesh=mesh,
        in_specs=(
            P("facet", None, None, "layer"),
            P("layer", "facet", None, None),
            P("facet", None),
            P("facet"),
            P(),
            P("layer", None),
            P("layer", "facet", None),
            P("layer", "facet", None),
            P("layer", "facet", None),
            P("layer", "facet", None, None),
        ),
        out_specs=(P("layer", "facet", None, None), P("facet", None, None, "layer")),
        check_vma=False,
    )
```

```python
import functools
import math

import jax
import jax.numpy as jnp
import numpy as np
from jax import lax
from jax.experimental import pallas as pl
from jax.experimental.pallas import tpu as pltpu
from jax.sharding import PartitionSpec as P

MESH = pl.DeviceIdType.MESH
BACK_GAIN = 8.0
CHUNKS = 8


def _fit(values, degree):
    nodes = np.cos(np.pi * (np.arange(64) + 0.5) / 64)
    y = (nodes + 1.0) * 0.5 * np.pi**2
    cheb = np.polynomial.chebyshev.Chebyshev.fit(y, values(np.sqrt(y)), degree, domain=[0, np.pi**2])
    return [float(v) for v in cheb.convert(kind=np.polynomial.Polynomial).coef]


COS = _fit(np.cos, 8)
SIN = _fit(lambda x: np.sinc(x / np.pi), 7)


def cos_sin(x):
    y = x * x
    c = jnp.full_like(y, COS[-1])
    for v in COS[-2::-1]:
        c = c * y + v
    s = jnp.full_like(y, SIN[-1])
    for v in SIN[-2::-1]:
        s = s * y + v
    return c, s * x


def dft(length):
    k = np.arange(length)
    angles = 2.0 * np.pi * ((k[:, None] * k[None, :]) % length) / length
    scale = 1.0 / math.sqrt(length)
    return np.cos(angles) * scale, -np.sin(angles) * scale


def barrier_line(i, n):
    sem = pltpu.get_barrier_semaphore()

    @pl.when(i > 0)
    def _():
        pl.semaphore_signal(sem, inc=1, device_id={"layer": i - 1}, device_id_type=MESH)

    @pl.when(i < n - 1)
    def _():
        pl.semaphore_signal(sem, inc=1, device_id={"layer": i + 1}, device_id_type=MESH)

    peers = jnp.where(i > 0, 1, 0) + jnp.where(i < n - 1, 1, 0)
    pl.semaphore_wait(sem, peers)


def forward_kernel(n, x_ref, ang_ref, f1_ref, g_ref, tw_ref, fac_ref, out_ref, buf, send_sem, recv_sem, own_sem):
    i = lax.axis_index("layer")
    cq = x_ref.shape[0] // CHUNKS
    subgrids = g_ref.shape[0] // 2
    rows = f1_ref.shape[0] // 2
    barrier_line(i, n)
    own = pltpu.make_async_copy(x_ref, buf.at[i], own_sem)
    own.start()

    def copy(direction, s, q):
        step = 1 if direction == 0 else -1
        origin = jnp.clip(i - step * s, 0, n - 1)
        cols = pl.ds(q * cq, cq)
        src = x_ref.at[cols] if s == 0 else buf.at[origin, cols]
        return pltpu.make_async_remote_copy(
            src_ref=src,
            dst_ref=buf.at[origin, cols],
            send_sem=send_sem.at[direction, s, q],
            recv_sem=recv_sem.at[direction, s, q],
            device_id={"layer": jnp.clip(i + step, 0, n - 1)},
            device_id_type=MESH,
        )

    def sends(direction, s):
        if direction == 0:
            return (i - s >= 0) & (i < n - 1)
        return (i + s <= n - 1) & (i > 0)

    def gets(direction, s):
        return i - 1 - s >= 0 if direction == 0 else i + 1 + s <= n - 1

    def compute(q):
        twr, twi = tw_ref[0], tw_ref[1]
        facr, faci = fac_ref[0], fac_ref[1]
        for pair in range(cq // 2):
            halves = []
            for c in (2 * pair, 2 * pair + 1):
                col = q * cq + c
                xr = jnp.concatenate([buf[l, col, 0] for l in range(n)], axis=0).astype(jnp.float32)
                xi = jnp.concatenate([buf[l, col, 1] for l in range(n)], axis=0).astype(jnp.float32)
                cosine, sine = cos_sin(ang_ref[col].astype(jnp.float32))
                x = jnp.concatenate([xr * cosine - xi * sine, xr * sine + xi * cosine], axis=0)
                h = jnp.dot(f1_ref[...], x.astype(jnp.bfloat16), preferred_element_type=jnp.float32)
                hr, hi = h[:rows], h[rows:]
                halves.append(
                    jnp.concatenate([hr * twr - hi * twi, hr * twi + hi * twr], axis=1).astype(jnp.bfloat16)
                )
            both = jnp.concatenate(halves, axis=0)
            spec = lax.dot_general(
                g_ref[...], both, (((1,), (1,)), ((), ())), preferred_element_type=jnp.float32
            )
            sr, si = spec[:subgrids], spec[subgrids:]
            at = q * (cq // 2) + pair
            out_ref[0, at] = (sr * facr - si * faci).astype(jnp.bfloat16)
            out_ref[1, at] = (sr * faci + si * facr).astype(jnp.bfloat16)

    def body(t, carry):
        @pl.when(t < CHUNKS)
        def _():
            for d in range(2):
                @pl.when(sends(d, 0))
                def _():
                    copy(d, 0, t).start()

        for s in range(n - 1):
            q = t - 1 - s
            @pl.when((q >= 0) & (q < CHUNKS))
            def _():
                for d in range(2):
                    @pl.when(gets(d, s))
                    def _():
                        copy(d, s, q).wait_recv()
                        if s + 1 < n - 1:
                            @pl.when(sends(d, s + 1))
                            def _():
                                copy(d, s + 1, q).start()

        @pl.when(t >= n - 1)
        def _():
            compute(t - (n - 1))

        return carry

    own.wait()
    lax.fori_loop(0, CHUNKS + n - 1, body, 0)

    def drain(q, carry):
        for d in range(2):
            for s in range(n - 1):
                @pl.when(sends(d, s))
                def _():
                    copy(d, s, q).wait_send()
        return carry

    lax.fori_loop(0, CHUNKS, drain, 0)


def backward_kernel(n, a_ref, ang_ref, g_ref, f2_ref, tw_ref, fac_ref, out_ref, term, sbuf, rbuf, send_sem, recv_sem):
    i = lax.axis_index("layer")
    cols = ang_ref.shape[0]
    cq = cols // CHUNKS
    fine = g_ref.shape[0] // 2
    rows = ang_ref.shape[1]
    part = rows // n
    barrier_line(i, n)

    def copy(direction, j, q):
        where = pl.ds(q * cq, cq)
        step = 1 if direction == 0 else -1
        return pltpu.make_async_remote_copy(
            src_ref=sbuf.at[direction, j, where],
            dst_ref=rbuf.at[direction, j, where],
            send_sem=send_sem.at[direction, j, q],
            recv_sem=recv_sem.at[direction, j, q],
            device_id={"layer": jnp.clip(i + step, 0, n - 1)},
            device_id_type=MESH,
        )

    def behind(direction):
        return i > 0 if direction == 0 else i < n - 1

    def compute(q):
        twr, twi = tw_ref[0], tw_ref[1]
        facr, faci = fac_ref[0], fac_ref[1]
        for pair in range(cq // 2):
            at = q * (cq // 2) + pair
            ar = a_ref[0, at].astype(jnp.float32)
            ai = a_ref[1, at].astype(jnp.float32)
            b = jnp.concatenate([ar * facr + ai * faci, ai * facr - ar * faci], axis=0).astype(jnp.bfloat16)
            h = jnp.dot(g_ref[...], b, preferred_element_type=jnp.float32)
            hr, hi = h[:fine], h[fine:]
            mixed = jnp.concatenate([hr * twr + hi * twi, hi * twr - hr * twi], axis=1).astype(jnp.bfloat16)
            image = lax.dot_general(
                f2_ref[...], mixed, (((1,), (1,)), ((), ())), preferred_element_type=jnp.float32
            )
            for c in range(2):
                col = q * cq + 2 * pair + c
                ir = image[2 * c * rows : (2 * c + 1) * rows]
                ii = image[(2 * c + 1) * rows : (2 * c + 2) * rows]
                cosine, sine = cos_sin(ang_ref[col].astype(jnp.float32))
                tr = (BACK_GAIN * (ir * cosine + ii * sine)).astype(jnp.bfloat16)
                ti = (BACK_GAIN * (ii * cosine - ir * sine)).astype(jnp.bfloat16)
                for l in range(n):
                    term[l, col, 0] = tr[l * part : (l + 1) * part]
                    term[l, col, 1] = ti[l * part : (l + 1) * part]

    def relay(direction, j, q):
        where = pl.ds(q * cq, cq)

        @pl.when(behind(direction))
        def _():
            copy(direction, j, q).wait_recv()
            total = term[j, where].astype(jnp.float32) + rbuf[direction, j, where].astype(jnp.float32)
            sbuf[direction, j, where] = total.astype(jnp.bfloat16)

        @pl.when(jnp.logical_not(behind(direction)))
        def _():
            sbuf[direction, j, where] = term[j, where]

        copy(direction, j, q).start()

    def body(t, carry):
        @pl.when(t < CHUNKS)
        def _():
            compute(t)

        for direction in range(2):
            q = t - i if direction == 0 else t - (n - 1 - i)

            @pl.when((q >= 0) & (q < CHUNKS))
            def _():
                for d in range(n - 1, 0, -1):
                    j = i + d if direction == 0 else i - d

                    @pl.when((j < n) & (j >= 0))
                    def _():
                        relay(direction, j, q)

        last = t - (n - 1)

        @pl.when(last >= 0)
        def _():
            where = pl.ds(last * cq, cq)
            out_ref[where] = term[i, where].astype(jnp.float32)
            for direction in range(2):
                @pl.when(behind(direction))
                def _():
                    copy(direction, i, last).wait_recv()
                    out_ref[where] += rbuf[direction, i, where].astype(jnp.float32)

        return carry

    lax.fori_loop(0, CHUNKS + n - 1, body, 0)

    def drain(q, carry):
        for direction in range(2):
            for d in range(1, n):
                j = i + d if direction == 0 else i - d

                @pl.when((j < n) & (j >= 0))
                def _():
                    copy(direction, j, q).wait_send()
        return carry

    lax.fori_loop(0, CHUNKS, drain, 0)


def facet_factor(window, shift_cells, subgrids):
    length = window.shape[0]
    rows = length // subgrids
    grid = window.reshape(subgrids, rows)
    grid = jnp.concatenate([grid, grid], axis=1)
    high = lax.broadcasted_iota(jnp.int32, grid.shape, 0)
    low = lax.broadcasted_iota(jnp.int32, grid.shape, 1) % rows
    turn_count = (high * rows + low) * shift_cells % length
    angles = 2.0 * math.pi / length * turn_count.astype(jnp.float32)
    return jnp.stack([grid * jnp.cos(angles), -grid * jnp.sin(angles)])


def spread(cells, length, taps):
    count = taps.shape[0]
    lanes = jnp.arange(length, dtype=jnp.int32)
    offset = (lanes - cells[..., None] + (count // 2 + length)) % length
    out = jnp.zeros(offset.shape, jnp.float32)
    for t in range(count):
        out = out + jnp.where(offset == t, taps[t], 0.0)
    return out


def middle(grids, u, v, plane, observed, angle, taps, rows, cols):
    row_weights = spread(u, rows, taps)
    column_weights = spread(v, cols, taps).astype(jnp.bfloat16)
    picked = jnp.einsum("sjc,sck->sjk", column_weights, grids.astype(jnp.bfloat16), preferred_element_type=jnp.float32)
    model_real = jnp.sum(picked[..., :rows] * row_weights, axis=2)
    model_imag = jnp.sum(picked[..., rows:] * row_weights, axis=2)
    pick = plane[..., None] == jnp.arange(angle.shape[0], dtype=jnp.int32)
    cosine = jnp.sum(jnp.where(pick, jnp.cos(angle), 0.0), axis=2)
    sine = jnp.sum(jnp.where(pick, jnp.sin(angle), 0.0), axis=2)
    res_real = observed[:, 0] - (model_real * cosine - model_imag * sine)
    res_imag = observed[:, 1] - (model_real * sine + model_imag * cosine)
    w_real = res_real * cosine + res_imag * sine
    w_imag = res_imag * cosine - res_real * sine
    spread_rows = jnp.concatenate(
        [w_real[..., None] * row_weights, w_imag[..., None] * row_weights], axis=2
    ).astype(jnp.bfloat16)
    adjoint = jnp.einsum("sjc,sjk->sck", column_weights, spread_rows, preferred_element_type=jnp.float32)
    return jnp.stack([res_real, res_imag], axis=1), adjoint.astype(jnp.bfloat16)


def middle_kernel(
    contrib_ref, u_ref, v_ref, plane_ref, obs_ref, taps_ref, table_ref, res_ref, out_ref,
    r0, acc0, r1, acc1, r2, fin, adj, phase, row_table, column_table, s0, d0, s1, d1, s2, d2, sg, dg,
):
    pairs = contrib_ref.shape[1]
    per, vis = u_ref.shape
    rows = contrib_ref.shape[3] // 2
    cols = 2 * pairs
    f = lax.axis_index("facet")
    core = lax.rem(f, 2)
    chip = lax.div(f, 2)
    bits = (lax.rem(chip, 2), lax.div(chip, 2))

    def flip(b):
        return f + (1 - 2 * bits[b]) * (2 * (1 + b))

    other = f + 1 - 2 * core
    barrier = pltpu.get_barrier_semaphore()
    for peer in (other, flip(0), flip(1)):
        pl.semaphore_signal(barrier, inc=1, device_id={"facet": peer}, device_id_type=MESH)
    pl.semaphore_wait(barrier, 3)

    def rows_of(device):
        return pl.ds(pl.multiple_of(device * per, per), per)

    def compose(p, along, across):
        return along + 2 * across if p == 0 else across + 2 * along

    def remote(src, dst, send, recv, device):
        return pltpu.make_async_remote_copy(
            src_ref=src, dst_ref=dst, send_sem=send, recv_sem=recv,
            device_id={"facet": device}, device_id_type=MESH,
        )

    def stage0(p, h):
        return remote(
            contrib_ref.at[p, :, rows_of(2 * h + 1 - core)], r0.at[p, h], s0.at[p, h], d0.at[p, h], other
        )

    def stage1(p, k):
        return remote(acc0.at[p, compose(p, 1 - bits[p], k)], r1.at[p, k], s1.at[p, k], d1.at[p, k], flip(p))

    def stage2(p):
        return remote(acc1.at[p, 1 - bits[1 - p]], r2.at[p], s2.at[p], d2.at[p], flip(1 - p))

    def add0(p, h):
        stage0(p, h).wait_recv()
        mine = contrib_ref[p, :, rows_of(2 * h + core)].astype(jnp.float32)
        acc0[p, h] = (mine + r0[p, h].astype(jnp.float32)).astype(jnp.bfloat16)

    order = [(a, k, p) for a in (1, 0) for k in range(2) for p in range(2)]
    for a, k, p in order:
        stage0(p, compose(p, 1 - bits[p] if a else bits[p], k)).start()
    for k in range(2):
        for p in range(2):
            add0(p, compose(p, 1 - bits[p], k))
            stage1(p, k).start()
    for k in range(2):
        for p in range(2):
            add0(p, compose(p, bits[p], k))

    plane = plane_ref[...]
    cosine = jnp.zeros(plane.shape, jnp.float32)
    sine = jnp.zeros(plane.shape, jnp.float32)
    for k in range(table_ref.shape[1]):
        hit = plane == k
        cosine = jnp.where(hit, table_ref[0, k], cosine)
        sine = jnp.where(hit, table_ref[1, k], sine)
    phase[0] = cosine
    phase[1] = sine

    def weights(cells, position, length):
        count = taps_ref.shape[0]
        offset = position - cells + count // 2
        offset = jnp.where(offset < 0, offset + length, jnp.where(offset >= length, offset - length, offset))
        out = jnp.zeros(offset.shape, jnp.float32)
        for t in range(count):
            out = jnp.where(offset == t, taps_ref[t], out)
        return out

    def prepare(s, carry):
        at = pl.ds(s, 1)
        row = lax.broadcasted_iota(jnp.int32, (rows, vis), 0)
        half = lax.broadcasted_iota(jnp.int32, (pairs, vis), 0)
        col = jnp.concatenate([2 * half, 2 * half + 1], axis=0)
        row_table[s] = weights(u_ref[at, :], row, rows)
        column_table[s] = weights(v_ref[at, :], col, cols).astype(jnp.bfloat16)
        return carry

    lax.fori_loop(0, per, prepare, 0)

    for k in range(2):
        for p in range(2):
            stage1(p, k).wait_recv()
            total = acc0[p, compose(p, bits[p], k)].astype(jnp.float32) + r1[p, k].astype(jnp.float32)
            acc1[p, k] = total.astype(jnp.bfloat16)
    for p in range(2):
        stage2(p).start()
    for p in range(2):
        stage2(p).wait_recv()
        for t in range(pairs):
            total = acc1[p, bits[1 - p], t].astype(jnp.float32) + r2[p, t].astype(jnp.float32)
            fin[p, pl.ds(t, per, stride=pairs), :] = total

    def one(s):
        at = pl.ds(s, 1)
        where = pl.ds(pl.multiple_of(s * pairs, pairs), pairs)
        row_weights = row_table[s]
        column_weights = column_table[s]
        real, imag = fin[0, where, :], fin[1, where, :]
        grid = jnp.concatenate(
            [
                jnp.concatenate([real[:, :rows], imag[:, :rows]], axis=1),
                jnp.concatenate([real[:, rows:], imag[:, rows:]], axis=1),
            ],
            axis=0,
        )
        picked = lax.dot_general(
            grid.astype(jnp.bfloat16), column_weights, (((0,), (0,)), ((), ())),
            preferred_element_type=jnp.float32,
        )
        model_real = jnp.sum(picked[:rows] * row_weights, axis=0, keepdims=True)
        model_imag = jnp.sum(picked[rows:] * row_weights, axis=0, keepdims=True)
        cosine, sine = phase[0, at, :], phase[1, at, :]
        res_real = obs_ref[s, 0:1, :] - (model_real * cosine - model_imag * sine)
        res_imag = obs_ref[s, 1:2, :] - (model_real * sine + model_imag * cosine)
        res_ref[s, 0:1, :] = res_real
        res_ref[s, 1:2, :] = res_imag
        w_real = res_real * cosine + res_imag * sine
        w_imag = res_imag * cosine - res_real * sine
        spread_rows = jnp.concatenate([row_weights * w_real, row_weights * w_imag], axis=0).astype(jnp.bfloat16)
        back = lax.dot_general(
            column_weights, spread_rows, (((1,), (1,)), ((), ())), preferred_element_type=jnp.float32
        )
        adj[0, where, :] = jnp.concatenate([back[:pairs, :rows], back[pairs:, :rows]], axis=1)
        adj[1, where, :] = jnp.concatenate([back[:pairs, rows:], back[pairs:, rows:]], axis=1)

    def four(block, carry):
        for k in range(4):
            one(4 * block + k)
        return carry

    lax.fori_loop(0, per // 4, four, 0)

    def gather(step, p, device, peer):
        block = out_ref.at[p, :, rows_of(device)]
        return remote(block, block, sg.at[step, p, device], dg.at[p, device], peer)

    def far(p, a, k):
        along = 1 - bits[p] if a else bits[p]
        across = 1 - bits[1 - p] if k else bits[1 - p]
        return 2 * compose(p, along, across) + core

    for p in range(2):
        for t in range(pairs):
            out_ref[p, t, rows_of(f)] = adj[p, pl.ds(t, per, stride=pairs), :].astype(jnp.bfloat16)
        gather(0, p, f, flip(1 - p)).start()
        gather(1, p, f, flip(p)).start()
        gather(2, p, f, other).start()
    for p in range(2):
        block = far(p, 0, 1)
        gather(0, p, block, flip(1 - p)).wait_recv()
        gather(1, p, block, flip(p)).start()
        gather(2, p, block, other).start()
    for k in range(2):
        for p in range(2):
            block = far(p, 1, k)
            gather(1, p, block, flip(p)).wait_recv()
            gather(2, p, block, other).start()
    for p in range(2):
        for h in range(4):
            gather(2, p, 2 * h + 1 - core, other).wait_recv()
    for p in range(2):
        for h in range(4):
            stage0(p, h).wait_send()
            gather(2, p, 2 * h + core, other).wait_send()
        for k in range(2):
            stage1(p, k).wait_send()
            gather(1, p, far(p, 0, k), flip(p)).wait_send()
        stage2(p).wait_send()
        gather(0, p, f, flip(1 - p)).wait_send()


def fused_middle(contrib, u, v, plane, observed, taps, table):
    _, pairs, subgrids, lanes = contrib.shape
    per, vis = u.shape
    vmem = pl.BlockSpec(memory_space=pltpu.VMEM)
    smem = pl.BlockSpec(memory_space=pltpu.SMEM)
    block = (pairs, per, lanes)
    wire = lambda *lead: pltpu.VMEM((*lead, *block), jnp.bfloat16)
    dma = lambda *shape: pltpu.SemaphoreType.DMA(shape)
    return pl.pallas_call(
        middle_kernel,
        out_shape=(
            jax.ShapeDtypeStruct((per, 2, vis), jnp.float32),
            jax.ShapeDtypeStruct(contrib.shape, jnp.bfloat16),
        ),
        in_specs=[vmem] * 5 + [smem] * 2,
        out_specs=(vmem, vmem),
        scratch_shapes=[
            wire(2, 4), wire(2, 4), wire(2, 2), wire(2, 2), wire(2),
            pltpu.VMEM((2, per * pairs, lanes), jnp.float32),
            pltpu.VMEM((2, per * pairs, lanes), jnp.float32),
            pltpu.VMEM((2, per, vis), jnp.float32),
            pltpu.VMEM((per, lanes // 2, vis), jnp.float32),
            pltpu.VMEM((per, 2 * pairs, vis), jnp.bfloat16),
            dma(2, 4), dma(2, 4), dma(2, 2), dma(2, 2), dma(2), dma(2), dma(3, 2, 8), dma(2, 8),
        ],
        compiler_params=pltpu.CompilerParams(collective_id=2, has_side_effects=True),
        name="degrid_exchange",
    )(contrib, u, v, plane, observed, taps, table)


def local(n, nf, model_strip, screen_angle, facet_window, facet_shift, kernel_taps, plane_angle, u_cell, v_cell, w_plane, observed):
    _, _, cols, length = screen_angle.shape
    per = u_cell.shape[1]
    subgrids = per * nf
    rows = length // subgrids
    block = rows // n
    vmem = pl.BlockSpec(memory_space=pltpu.VMEM)
    fr, fi = dft(rows)
    gr, gi = dft(subgrids)
    turn = 2.0 * np.pi * (np.arange(rows)[:, None] * np.arange(subgrids)[None, :] % length) / length
    twist = np.stack([np.cos(turn), -np.sin(turn)]).astype(np.float32)
    bf = lambda a: jnp.asarray(a.astype(np.float32)).astype(jnp.bfloat16)
    f1 = bf(np.block([[fr, -fi], [fi, fr]]))
    g1 = bf(np.block([[gr, -gi], [gi, gr]]))
    g2 = bf(np.block([[gr.T, gi.T], [-gi.T, gr.T]]))
    zero = np.zeros_like(fr)
    f2 = bf(
        np.block(
            [
                [fr.T, zero, fi.T, zero],
                [-fi.T, zero, fr.T, zero],
                [zero, fr.T, zero, fi.T],
                [zero, -fi.T, zero, fr.T],
            ]
        )
    )
    tw2 = np.ascontiguousarray(np.tile(np.swapaxes(twist, 1, 2), (1, 1, 2)))
    factor = facet_factor(facet_window[0], facet_shift[0], subgrids)
    x = model_strip[0].reshape(2, cols, block, subgrids).transpose(1, 0, 2, 3)
    angle = screen_angle[0, 0].reshape(cols, rows, subgrids)
    contrib = pl.pallas_call(
        functools.partial(forward_kernel, n),
        out_shape=jax.ShapeDtypeStruct((2, cols // 2, subgrids, 2 * rows), jnp.bfloat16),
        in_specs=[vmem] * 6,
        out_specs=vmem,
        scratch_shapes=[
            pltpu.VMEM((n, cols, 2, block, subgrids), jnp.bfloat16),
            pltpu.SemaphoreType.DMA((2, n - 1, CHUNKS)),
            pltpu.SemaphoreType.DMA((2, n - 1, CHUNKS)),
            pltpu.SemaphoreType.DMA,
        ],
        compiler_params=pltpu.CompilerParams(collective_id=0, has_side_effects=True),
        name="gather_forward",
    )(x, angle, f1, g1, jnp.asarray(twist), factor)
    if nf == 8 and per % 16 == 0:
        table = jnp.stack([jnp.cos(plane_angle[0]), jnp.sin(plane_angle[0])])
        residual, every = fused_middle(
            contrib, u_cell[0], v_cell[0], w_plane[0], observed[0], kernel_taps, table
        )
    else:
        parts = contrib.reshape(2, cols // 2, nf, per, 2 * rows)
        received = lax.all_to_all(parts, "facet", split_axis=2, concat_axis=2, tiled=True)
        grids = jnp.sum(received.astype(jnp.float32), axis=2)
        grids = grids.reshape(2, cols // 2, per, 2, rows).transpose(2, 1, 3, 0, 4).reshape(per, cols, 2 * rows)
        residual, adjoint = middle(
            grids, u_cell[0], v_cell[0], w_plane[0], observed[0], plane_angle[0], kernel_taps, rows, cols
        )
        adjoint = adjoint.reshape(per, cols // 2, 2, 2, rows).transpose(3, 1, 0, 2, 4).reshape(2, cols // 2, per, 2 * rows)
        every = lax.all_gather(adjoint, "facet", axis=2, tiled=True)
    gradient = pl.pallas_call(
        functools.partial(backward_kernel, n),
        out_shape=jax.ShapeDtypeStruct((cols, 2, block, subgrids), jnp.float32),
        in_specs=[vmem] * 6,
        out_specs=vmem,
        scratch_shapes=[
            pltpu.VMEM((n, cols, 2, block, subgrids), jnp.bfloat16),
            pltpu.VMEM((2, n, cols, 2, block, subgrids), jnp.bfloat16),
            pltpu.VMEM((2, n, cols, 2, block, subgrids), jnp.bfloat16),
            pltpu.SemaphoreType.DMA((2, n, CHUNKS)),
            pltpu.SemaphoreType.DMA((2, n, CHUNKS)),
        ],
        compiler_params=pltpu.CompilerParams(collective_id=1, has_side_effects=True),
        name="backward_scatter",
    )(every, angle, g2, f2, jnp.asarray(tw2), factor)
    gradient = gradient.transpose(1, 0, 2, 3).reshape(1, 2, cols, block * subgrids)
    return (residual[None], gradient)


def solution(mesh):
    return jax.shard_map(
        functools.partial(local, mesh.shape["layer"], mesh.shape["facet"]),
        mesh=mesh,
        in_specs=(
            P("facet", None, None, "layer"),
            P("layer", "facet", None, None),
            P("facet", None),
            P("facet"),
            P(),
            P("layer", None),
            P("layer", "facet", None),
            P("layer", "facet", None),
            P("layer", "facet", None),
            P("layer", "facet", None, None),
        ),
        out_specs=(P("layer", "facet", None, None), P("facet", None, None, "layer")),
        check_vma=False,
    )
```
